32 devices in a mesh: gx: 8 (over y, x, core), gy: 4 (over z).
Axes of the slice: x: 2, y: 2, z: 4, core: 2. Of those that a mesh axis runs over, the one named last changes fastest.
Arguments:
- basis: float32 [32, 128, 64, 256], P(None, 'gx', 'gy'), may hold values from -0.09375 to 0.09375
- reaction: float32 [128, 64, 256], P('gx', 'gy'), may hold values from 0.5 to 4
Outputs:
- extended: float32 [32, 128, 64, 256], P(None, 'gx', 'gy')
- coarse: float32 [32, 5, 32, 32], replicated
The draws below stay inside these ranges and needn't reach their ends.
All inputs are finite; a program needn't handle non-finite values.
Results may differ from the reference program's by a relative error of at most 0.000071.
Values sent between devices are 32-bit elements; how exact they have to be, the bound alone decides.
A program may use at most 128 MiB of HBM per device.

```python
import math
import jax
import jax.numpy as jnp
from jax import lax

K = 32
SWEEPS = 4
CX = 16
CY = 16
CZ = 256
NX = 128
NY = 64
N_GX = 8
N_GY = 4


def level_of(rng, extent, shards, smallest, high):
    factor_of, own = 1.0, jax.random.fold_in(rng, 6)
    for axis_at, blocks in shards:
        draws = jnp.exp(jax.random.uniform(jax.random.fold_in(own, axis_at), (blocks,), jnp.float32, smallest / len(shards), high / len(shards)))
        factor_of = factor_of * jnp.repeat(draws, extent[axis_at] // blocks).reshape([-1 if axis == axis_at else 1 for axis in range(len(extent))])
    return factor_of


def centred(rng, extent, width, limit, shards=(), dtype=jnp.bfloat16):
    loudness = level_of(rng, extent, shards, -0.22, 0.18) if shards else 1.0
    result = jax.random.normal(rng, extent, jnp.float32) * width * loudness
    return jnp.minimum(jnp.maximum(result, -limit), limit).astype(dtype)


def setup_inputs(seed: int = 0) -> dict:
    keys = jax.random.split(jax.random.key(seed), 3)
    basis = centred(keys[0], (K, NX, NY, CZ), (CY * CZ) ** -0.5, 0.09375, ((1, 8), (2, 4)), jnp.float32)
    reaction = jnp.clip(jnp.exp(math.log(4.0) - 2.0794415 * jax.random.uniform(keys[1], (NX, NY, CZ), jnp.float32) ** level_of(keys[1], (NX, NY, CZ), ((0, 8), (1, 4)), -0.2, 0.2)), 0.5, 4.0)
    return dict(basis=basis, reaction=reaction)


OMEGA = 0.8


def stencil(field, coef):
    padded = jnp.pad(field, ((0, 0), (1, 1), (1, 1), (1, 1)))
    beside = padded[:, 2:, 1:-1, 1:-1] + padded[:, :-2, 1:-1, 1:-1]
    beside = beside + padded[:, 1:-1, 2:, 1:-1] + padded[:, 1:-1, :-2, 1:-1]
    beside = beside + padded[:, 1:-1, 1:-1, 2:] + padded[:, 1:-1, 1:-1, :-2]
    return (6.0 + coef) * field - beside


def extend_one(pair):
    phi, coef = pair
    kk, cx, cy, cz = phi.shape
    xpos = lax.broadcasted_iota(jnp.int32, (cx, cy, cz), 0)
    ypos = lax.broadcasted_iota(jnp.int32, (cx, cy, cz), 1)
    inner = (xpos >= 1) & (xpos <= cx - 2) & (ypos >= 1) & (ypos <= cy - 2)
    for sweep in range(SWEEPS):
        update = OMEGA * stencil(phi, coef) / (6.0 + coef)
        phi = phi - jnp.where(inner[None], update, jnp.float32(0.0))
    applied = stencil(phi, coef)
    diag = jnp.dot(phi.reshape(kk, -1), applied.reshape(kk, -1).T,
                   precision=lax.Precision.HIGHEST, preferred_element_type=jnp.float32)
    return phi, diag


def couple(own, other):
    return -jnp.einsum("iabyz,jabyz->abij", own, other, precision=lax.Precision.HIGHEST)


def reference(basis, reaction):
    gxn, gyn = N_GX, N_GY
    blocked = basis.reshape(K, gxn, CX, gyn, CY, CZ)
    subs = blocked.transpose(1, 3, 0, 2, 4, 5).reshape(gxn * gyn, K, CX, CY, CZ)
    coefs = reaction.reshape(gxn, CX, gyn, CY, CZ).transpose(0, 2, 1, 3, 4).reshape(gxn * gyn, CX, CY, CZ)
    phis, diags = lax.map(extend_one, (subs, coefs))
    extended = phis.reshape(gxn, gyn, K, CX, CY, CZ).transpose(2, 0, 3, 1, 4, 5).reshape(K, gxn * CX, gyn * CY, CZ)
    low_x = blocked[:, :, 0]
    high_x = blocked[:, :, CX - 1]
    zero_x = jnp.zeros_like(low_x[:, :1])
    minus_x = couple(low_x, jnp.concatenate([zero_x, high_x[:, :-1]], axis=1))
    plus_x = couple(high_x, jnp.concatenate([low_x[:, 1:], zero_x], axis=1))
    low_y = blocked[:, :, :, :, 0].transpose(0, 1, 3, 2, 4)
    high_y = blocked[:, :, :, :, CY - 1].transpose(0, 1, 3, 2, 4)
    zero_y = jnp.zeros_like(low_y[:, :, :1])
    minus_y = couple(low_y, jnp.concatenate([zero_y, high_y[:, :, :-1]], axis=2))
    plus_y = couple(high_y, jnp.concatenate([low_y[:, :, 1:], zero_y], axis=2))
    count = gxn * gyn
    coarse = jnp.stack([diags, minus_x.reshape(count, K, K), plus_x.reshape(count, K, K),
                        minus_y.reshape(count, K, K), plus_y.reshape(count, K, K)], axis=1)
    return extended, coarse
```

```python
import functools

import jax
import jax.numpy as jnp
from jax import lax
from jax.experimental import pallas as pl
from jax.experimental.pallas import tpu as pltpu
from jax.sharding import PartitionSpec as P

SWEEPS = 4
OMEGA = 0.8
GROUP = 8
LANES = 128


def passed_along(block, axis, distance):
    devices = range(lax.axis_size(axis))
    route = [(i - distance, i) for i in devices if i - distance in devices]
    return lax.ppermute(block, axis, route)


def along_z(field, lane):
    zero = jnp.zeros_like(field[0])
    back = [pltpu.roll(piece, 1, 1) for piece in field]
    ahead = [pltpu.roll(piece, LANES - 1, 1) for piece in field]
    sums = []
    for h in range(len(field)):
        below = jnp.where(lane == 0, back[h - 1] if h else zero, back[h])
        above = jnp.where(lane == LANES - 1, ahead[h + 1] if h + 1 < len(field) else zero, ahead[h])
        sums.append(below + above)
    return sums


def pieces(ref, x, y):
    parts = ref.shape[-1] // LANES
    return [ref[x, y, :, h * LANES:(h + 1) * LANES] for h in range(parts)]


def halves(value):
    high = value.astype(jnp.bfloat16).astype(jnp.float32)
    return jnp.concatenate([value, value - high], axis=0).astype(jnp.bfloat16)


def extend_kernel(basis, reaction, extended, product, first, second, weight, centre, left, right):
    _, cx, cy, cz = basis.shape
    parts = cz // LANES
    group = pl.program_id(0)
    lane = lax.broadcasted_iota(jnp.int32, (GROUP, LANES), 1)

    @pl.when(group == 0)
    def _():
        blank = jnp.zeros((cy, GROUP, cz), jnp.float32)
        for buffer in (first,):
            buffer[0] = blank
            buffer[cx + 1] = blank

        @pl.loop(0, cx)
        def _(x):
            whole = 6.0 + reaction[x]
            scaled = OMEGA / whole
            for y in range(cy):
                centre[x, y] = jnp.broadcast_to(whole[y:y + 1], (GROUP, cz))
                weight[x, y] = jnp.broadcast_to(scaled[y:y + 1], (GROUP, cz))

    @pl.loop(0, cx)
    def _(x):
        for y in range(0, cy, GROUP):
            turned = jnp.swapaxes(basis[:, x, y:y + GROUP, :], 0, 1)
            first[x + 1, y:y + GROUP] = turned
            if y == 0:
                second[x + 1, 0] = turned[0]
            if y == cy - GROUP:
                second[x + 1, cy - 1] = turned[GROUP - 1]

    second[1] = first[1]
    second[cx] = first[cx]

    buffers = (first, second)
    for sweep in range(SWEEPS):
        source, target = buffers[sweep % 2], buffers[(sweep + 1) % 2]

        @pl.loop(2, cx)
        def _(x):
            before, here = pieces(source, x, 0), pieces(source, x, 1)
            for y in range(1, cy - 1):
                after = pieces(source, x, y + 1)
                down, up = pieces(source, x - 1, y), pieces(source, x + 1, y)
                scale = pieces(weight, x - 1, y)
                beside = along_z(here, lane)
                for h in range(parts):
                    total = (down[h] + up[h]) + (before[h] + after[h]) + beside[h]
                    target[x, y, :, h * LANES:(h + 1) * LANES] = (
                        (1.0 - OMEGA) * here[h] + scale[h] * total
                    )
                before, here = here, after

    final = buffers[SWEEPS % 2]
    rows = pl.ds(pl.multiple_of(group * 2 * GROUP, 2 * GROUP), 2 * GROUP)

    @pl.loop(1, cx + 1)
    def _(x):
        before, here = None, pieces(final, x, 0)
        for y in range(cy):
            after = pieces(final, x, y + 1) if y + 1 < cy else None
            down, up = pieces(final, x - 1, y), pieces(final, x + 1, y)
            whole = pieces(centre, x - 1, y)
            beside = along_z(here, lane)
            for h in range(parts):
                total = (down[h] + up[h]) + beside[h]
                if before is not None:
                    total = total + before[h]
                if after is not None:
                    total = total + after[h]
                applied = whole[h] * here[h] - total
                left[x - 1, y * parts + h, rows, :] = halves(here[h])
                right[x - 1, y * parts + h, rows, :] = halves(applied)
            before, here = here, after
        for y in range(0, cy, GROUP):
            extended[:, x - 1, y:y + GROUP, :] = jnp.swapaxes(final[x, y:y + GROUP], 0, 1)

    @pl.when(group == pl.num_programs(0) - 1)
    def _():
        def add(x, total):
            one = jnp.concatenate([left[x, i] for i in range(cy * parts)], axis=1)
            other = jnp.concatenate([right[x, i] for i in range(cy * parts)], axis=1)
            return total + lax.dot_general(
                one, other, (((1,), (1,)), ((), ())), preferred_element_type=jnp.float32
            )

        size = product.shape[0]
        product[...] = lax.fori_loop(0, cx, add, jnp.zeros((size, size), jnp.float32))


def extend(basis, reaction):
    width, cx, cy, cz = basis.shape
    field = (cx + 2, cy, GROUP, cz)
    factors = pltpu.VMEM((cx, cy * cz // LANES, 2 * width, LANES), jnp.bfloat16)
    block = pl.BlockSpec((GROUP, cx, cy, cz), lambda g: (g, 0, 0, 0))
    return pl.pallas_call(
        extend_kernel,
        grid=(width // GROUP,),
        in_specs=[block, pl.BlockSpec((cx, cy, cz), lambda g: (0, 0, 0))],
        out_specs=[block, pl.BlockSpec((2 * width, 2 * width), lambda g: (0, 0))],
        out_shape=[
            jax.ShapeDtypeStruct(basis.shape, jnp.float32),
            jax.ShapeDtypeStruct((2 * width, 2 * width), jnp.float32),
        ],
        scratch_shapes=[
            pltpu.VMEM(field, jnp.float32),
            pltpu.VMEM(field, jnp.float32),
            pltpu.VMEM((cx, cy, GROUP, cz), jnp.float32),
            pltpu.VMEM((cx, cy, GROUP, cz), jnp.float32),
            factors,
            factors,
        ],
        compiler_params=pltpu.CompilerParams(vmem_limit_bytes=56 * 2**20),
        cost_estimate=pl.CostEstimate(
            flops=60 * basis.size, bytes_accessed=8 * basis.size, transcendentals=0
        ),
    )(basis, reaction)


def couple(own, other):
    width = own.shape[0]
    return -jnp.dot(
        own.reshape(width, -1),
        other.reshape(width, -1).T,
        precision=lax.Precision.HIGHEST,
        preferred_element_type=jnp.float32,
    )


def on_device(basis, reaction):
    width = basis.shape[0]
    right_face = passed_along(basis[:, 0], "gx", -1)
    upper_face = passed_along(basis[:, :, 0], "gy", -1)
    phi, product = extend(basis, reaction)
    groups = width // GROUP
    diag = product.reshape(groups, 2, GROUP, groups, 2, GROUP).sum((1, 4)).reshape(width, width)
    blocks = jnp.stack(
        [diag, couple(basis[:, -1], right_face), couple(basis[:, :, -1], upper_face)]
    )
    gathered = lax.all_gather(blocks[None], ("gx", "gy"), axis=0, tiled=True)
    columns = lax.axis_size("gy")
    plus_x = gathered[:, 1]
    plus_y = gathered[:, 2]
    minus_x = jnp.concatenate(
        [jnp.zeros((columns, width, width), jnp.float32), jnp.swapaxes(plus_x[:-columns], 1, 2)],
        axis=0,
    )
    minus_y = jnp.concatenate(
        [jnp.zeros((1, width, width), jnp.float32), jnp.swapaxes(plus_y[:-1], 1, 2)], axis=0
    )
    coarse = jnp.stack([gathered[:, 0], minus_x, plus_x, minus_y, plus_y], axis=1)
    return (phi, coarse)


def solution(mesh):
    placed = (P(None, "gx", "gy", None), P("gx", "gy", None))
    return jax.shard_map(
        on_device,
        mesh=mesh,
        in_specs=placed,
        out_specs=(P(None, "gx", "gy", None), P()),
        check_vma=False,
    )
```

```python
import functools

import jax
import jax.numpy as jnp
from jax import lax
from jax.experimental import pallas as pl
from jax.experimental.pallas import tpu as pltpu
from jax.sharding import PartitionSpec as P

SWEEPS = 4
OMEGA = 0.8
GROUP = 8
LANES = 128


def passed_along(block, axis, distance):
    devices = range(lax.axis_size(axis))
    route = [(i - distance, i) for i in devices if i - distance in devices]
    return lax.ppermute(block, axis, route)


def along_z(field, lane):
    zero = jnp.zeros_like(field[0])
    back = [pltpu.roll(piece, 1, 1) for piece in field]
    ahead = [pltpu.roll(piece, LANES - 1, 1) for piece in field]
    sums = []
    for h in range(len(field)):
        below = jnp.where(lane == 0, back[h - 1] if h else zero, back[h])
        above = jnp.where(lane == LANES - 1, ahead[h + 1] if h + 1 < len(field) else zero, ahead[h])
        sums.append(below + above)
    return sums


def pieces(ref, x, y):
    parts = ref.shape[-1] // LANES
    return [ref[x, y, :, h * LANES:(h + 1) * LANES] for h in range(parts)]


def halves(value):
    high = value.astype(jnp.bfloat16).astype(jnp.float32)
    return jnp.concatenate([value, value - high], axis=0).astype(jnp.bfloat16)


def extend_kernel(basis, reaction, extended, product, first, second, weight, centre, left, right):
    _, cx, cy, cz = basis.shape
    parts = cz // LANES
    group = pl.program_id(0)
    lane = lax.broadcasted_iota(jnp.int32, (GROUP, LANES), 1)

    @pl.when(group == 0)
    def _():
        blank = jnp.zeros((cy, GROUP, cz), jnp.float32)
        for buffer in (first,):
            buffer[0] = blank
            buffer[cx + 1] = blank

        @pl.loop(0, cx)
        def _(x):
            whole = 6.0 + reaction[x]
            scaled = OMEGA / whole
            for y in range(cy):
                centre[x, y] = jnp.broadcast_to(whole[y:y + 1], (GROUP, cz))
                weight[x, y] = jnp.broadcast_to(scaled[y:y + 1], (GROUP, cz))

    @pl.loop(0, cx)
    def _(x):
        for y in range(0, cy, GROUP):
            turned = jnp.swapaxes(basis[:, x, y:y + GROUP, :], 0, 1)
            first[x + 1, y:y + GROUP] = turned
            if y == 0:
                second[x + 1, 0] = turned[0]
            if y == cy - GROUP:
                second[x + 1, cy - 1] = turned[GROUP - 1]

    second[1] = first[1]
    second[cx] = first[cx]

    buffers = (first, second)
    for sweep in range(SWEEPS):
        source, target = buffers[sweep % 2], buffers[(sweep + 1) % 2]

        @pl.loop(2, cx)
        def _(x):
            before, here = pieces(source, x, 0), pieces(source, x, 1)
            for y in range(1, cy - 1):
                after = pieces(source, x, y + 1)
                down, up = pieces(source, x - 1, y), pieces(source, x + 1, y)
                scale = pieces(weight, x - 1, y)
                beside = along_z(here, lane)
                for h in range(parts):
                    total = (down[h] + up[h]) + (before[h] + after[h]) + beside[h]
                    target[x, y, :, h * LANES:(h + 1) * LANES] = (
                        (1.0 - OMEGA) * here[h] + scale[h] * total
                    )
                before, here = here, after

    final = buffers[SWEEPS % 2]
    rows = pl.ds(pl.multiple_of(group * 2 * GROUP, 2 * GROUP), 2 * GROUP)

    @pl.loop(1, cx + 1)
    def _(x):
        before, here = None, pieces(final, x, 0)
        for y in range(cy):
            after = pieces(final, x, y + 1) if y + 1 < cy else None
            down, up = pieces(final, x - 1, y), pieces(final, x + 1, y)
            whole = pieces(centre, x - 1, y)
            beside = along_z(here, lane)
            for h in range(parts):
                total = (down[h] + up[h]) + beside[h]
                if before is not None:
                    total = total + before[h]
                if after is not None:
                    total = total + after[h]
                applied = whole[h] * here[h] - total
                left[x - 1, y * parts + h, rows, :] = halves(here[h])
                right[x - 1, y * parts + h, rows, :] = halves(applied)
            before, here = here, after
        for y in range(0, cy, GROUP):
            extended[:, x - 1, y:y + GROUP, :] = jnp.swapaxes(final[x, y:y + GROUP], 0, 1)

    @pl.when(group == pl.num_programs(0) - 1)
    def _():
        def add(x, total):
            one = jnp.concatenate([left[x, i] for i in range(cy * parts)], axis=1)
            other = jnp.concatenate([right[x, i] for i in range(cy * parts)], axis=1)
            return total + lax.dot_general(
                one, other, (((1,), (1,)), ((), ())), preferred_element_type=jnp.float32
            )

        size = product.shape[0]
        product[...] = lax.fori_loop(0, cx, add, jnp.zeros((size, size), jnp.float32))


def extend(basis, reaction):
    width, cx, cy, cz = basis.shape
    field = (cx + 2, cy, GROUP, cz)
    factors = pltpu.VMEM((cx, cy * cz // LANES, 2 * width, LANES), jnp.bfloat16)
    block = pl.BlockSpec((GROUP, cx, cy, cz), lambda g: (g, 0, 0, 0))
    return pl.pallas_call(
        extend_kernel,
        grid=(width // GROUP,),
        in_specs=[block, pl.BlockSpec((cx, cy, cz), lambda g: (0, 0, 0))],
        out_specs=[block, pl.BlockSpec((2 * width, 2 * width), lambda g: (0, 0))],
        out_shape=[
            jax.ShapeDtypeStruct(basis.shape, jnp.float32),
            jax.ShapeDtypeStruct((2 * width, 2 * width), jnp.float32),
        ],
        scratch_shapes=[
            pltpu.VMEM(field, jnp.float32),
            pltpu.VMEM(field, jnp.float32),
            pltpu.VMEM((cx, cy, GROUP, cz), jnp.float32),
            pltpu.VMEM((cx, cy, GROUP, cz), jnp.float32),
            factors,
            factors,
        ],
        compiler_params=pltpu.CompilerParams(vmem_limit_bytes=56 * 2**20),
        cost_estimate=pl.CostEstimate(
            flops=60 * basis.size, bytes_accessed=8 * basis.size, transcendentals=0
        ),
    )(basis, reaction)


def couple(own, other):
    width = own.shape[0]
    return -jnp.dot(
        own.reshape(width, -1),
        other.reshape(width, -1).T,
        precision=lax.Precision.HIGHEST,
        preferred_element_type=jnp.float32,
    )


def packed(block):
    rows = block.shape[0] * block.shape[1] // LANES
    return jnp.concatenate(
        [block[i:i + rows] for i in range(0, block.shape[0], rows)], axis=1
    )


def unpacked(tile, width):
    return jnp.concatenate(
        [tile[:, i:i + width] for i in range(0, LANES, width)], axis=0
    )


def spread_kernel(ngx, ngy, product, plus_x, plus_y, coarse, held, send_y, recv_y, send_x, recv_x):
    gx, gy = lax.axis_index("gx"), lax.axis_index("gy")
    width = plus_x.shape[0]

    barrier = pltpu.get_barrier_semaphore()
    for d in range(1, ngy):
        pl.semaphore_signal(
            barrier, inc=1, device_id=(gx, lax.rem(gy + d, ngy)), device_id_type=pl.DeviceIdType.MESH
        )
    for d in range(1, ngx):
        pl.semaphore_signal(
            barrier, inc=1, device_id=(lax.rem(gx + d, ngx), gy), device_id_type=pl.DeviceIdType.MESH
        )

    span = 2 * GROUP
    rows = jnp.concatenate(
        [product[i:i + GROUP] + product[i + GROUP:i + span] for i in range(0, 2 * width, span)], axis=0
    )
    diag = jnp.concatenate(
        [rows[:, i:i + GROUP] + rows[:, i + GROUP:i + span] for i in range(0, 2 * width, span)], axis=1
    )
    held[gx, gy, 0] = packed(diag)
    held[gx, gy, 1] = packed(plus_x[...])
    held[gx, gy, 2] = packed(plus_y[...])
    for y in range(ngy):
        coarse[y, 1] = jnp.zeros((width, width), jnp.float32)
    coarse[0, 3] = jnp.zeros((width, width), jnp.float32)
    pl.semaphore_wait(barrier, ngx + ngy - 2)

    def over_y(owner, peer):
        piece = held.at[gx, owner]
        return pltpu.make_async_remote_copy(
            src_ref=piece, dst_ref=piece, send_sem=send_y.at[peer], recv_sem=recv_y.at[owner],
            device_id=(gx, peer), device_id_type=pl.DeviceIdType.MESH,
        )

    def over_x(row, owner, peer):
        piece = held.at[row, owner]
        return pltpu.make_async_remote_copy(
            src_ref=piece, dst_ref=piece, send_sem=send_x.at[peer, owner], recv_sem=recv_x.at[row, owner],
            device_id=(peer, gy), device_id_type=pl.DeviceIdType.MESH,
        )

    def unpack(row, owner):
        s = row * ngy + owner
        along_x, along_y = unpacked(held[row, owner, 1], width), unpacked(held[row, owner, 2], width)
        coarse[s, 0] = unpacked(held[row, owner, 0], width)
        coarse[s, 2] = along_x
        coarse[s, 4] = along_y

        @pl.when(row < ngx - 1)
        def _():
            coarse[s + ngy, 1] = along_x.T

        @pl.when(s < ngx * ngy - 1)
        def _():
            coarse[s + 1, 3] = along_y.T

    for d in range(1, ngy):
        over_y(gy, lax.rem(gy + d, ngy)).start()
    for d in range(1, ngx):
        over_x(gx, gy, lax.rem(gx + d, ngx)).start()
    for d in range(1, ngy):
        owner = lax.rem(gy + d, ngy)
        over_y(owner, owner).wait_recv()
        for e in range(1, ngx):
            over_x(gx, owner, lax.rem(gx + e, ngx)).start()

    @pl.loop(0, ngy)
    def _(owner):
        unpack(gx, owner)

    @pl.loop(0, ngy)
    def _(d):
        owner = lax.rem(gy + d, ngy)

        @pl.loop(1, ngx)
        def _(e):
            row = lax.rem(gx + e, ngx)
            over_x(row, owner, row).wait_recv()
            unpack(row, owner)

    for d in range(1, ngy):
        over_y(gy, lax.rem(gy + d, ngy)).wait_send()
    for d in range(ngy):
        owner = lax.rem(gy + d, ngy)
        for e in range(1, ngx):
            over_x(gx, owner, lax.rem(gx + e, ngx)).wait_send()


def spread(product, plus_x, plus_y):
    ngx, ngy = lax.axis_size("gx"), lax.axis_size("gy")
    width = plus_x.shape[0]
    vmem = pl.BlockSpec(memory_space=pltpu.VMEM)
    return pl.pallas_call(
        functools.partial(spread_kernel, ngx, ngy),
        in_specs=[vmem] * 3,
        out_specs=vmem,
        out_shape=jax.ShapeDtypeStruct((ngx * ngy, 5, width, width), jnp.float32),
        scratch_shapes=[
            pltpu.VMEM((ngx, ngy, 3, width * width // LANES, LANES), jnp.float32),
            pltpu.SemaphoreType.DMA((ngy,)),
            pltpu.SemaphoreType.DMA((ngy,)),
            pltpu.SemaphoreType.DMA((ngx, ngy)),
            pltpu.SemaphoreType.DMA((ngx, ngy)),
        ],
        compiler_params=pltpu.CompilerParams(collective_id=0, has_side_effects=True),
    )(product, plus_x, plus_y)


def on_device(basis, reaction):
    right_face = passed_along(basis[:, 0], "gx", -1)
    upper_face = passed_along(basis[:, :, 0], "gy", -1)
    phi, product = extend(basis, reaction)
    plus_x = couple(basis[:, -1], right_face)
    plus_y = couple(basis[:, :, -1], upper_face)
    return (phi, spread(product, plus_x, plus_y))


def solution(mesh):
    placed = (P(None, "gx", "gy", None), P("gx", "gy", None))
    return jax.shard_map(
        on_device,
        mesh=mesh,
        in_specs=placed,
        out_specs=(P(None, "gx", "gy", None), P()),
        check_vma=False,
    )
```

```python
import functools

import jax
import jax.numpy as jnp
from jax import lax
from jax.experimental import pallas as pl
from jax.experimental.pallas import tpu as pltpu
from jax.sharding import PartitionSpec as P

SWEEPS = 4
OMEGA = 0.8
GROUP = 8
LANES = 128


def passed_along(block, axis, distance):
    devices = range(lax.axis_size(axis))
    route = [(i - distance, i) for i in devices if i - distance in devices]
    return lax.ppermute(block, axis, route)


def along_z(field, lane):
    zero = jnp.zeros_like(field[0])
    back = [pltpu.roll(piece, 1, 1) for piece in field]
    ahead = [pltpu.roll(piece, LANES - 1, 1) for piece in field]
    sums = []
    for h in range(len(field)):
        below = jnp.where(lane == 0, back[h - 1] if h else zero, back[h])
        above = jnp.where(lane == LANES - 1, ahead[h + 1] if h + 1 < len(field) else zero, ahead[h])
        sums.append(below + above)
    return sums


def pieces(ref, x, y):
    parts = ref.shape[-1] // LANES
    return [ref[x, y, :, h * LANES:(h + 1) * LANES] for h in range(parts)]


def halves(value):
    high = value.astype(jnp.bfloat16).astype(jnp.float32)
    return jnp.concatenate([value, value - high], axis=0).astype(jnp.bfloat16)


def extend_kernel(basis, reaction, extended, product, upper, first, second, weight, centre, left, right):
    _, cx, cy, cz = basis.shape
    parts = cz // LANES
    group = pl.program_id(0)
    lane = lax.broadcasted_iota(jnp.int32, (GROUP, LANES), 1)

    @pl.when(group == 0)
    def _():
        blank = jnp.zeros((cy, GROUP, cz), jnp.float32)
        for buffer in (first,):
            buffer[0] = blank
            buffer[cx + 1] = blank

        @pl.loop(0, cx)
        def _(x):
            whole = 6.0 + reaction[x]
            scaled = OMEGA / whole
            for y in range(cy):
                centre[x, y] = jnp.broadcast_to(whole[y:y + 1], (GROUP, cz))
                weight[x, y] = jnp.broadcast_to(scaled[y:y + 1], (GROUP, cz))

    @pl.loop(0, cx)
    def _(x):
        for y in range(0, cy, GROUP):
            turned = jnp.swapaxes(basis[:, x, y:y + GROUP, :], 0, 1)
            first[x + 1, y:y + GROUP] = turned
            if y == 0:
                second[x + 1, 0] = turned[0]
            if y == cy - GROUP:
                second[x + 1, cy - 1] = turned[GROUP - 1]

    second[1] = first[1]
    second[cx] = first[cx]

    buffers = (first, second)
    for sweep in range(SWEEPS):
        source, target = buffers[sweep % 2], buffers[(sweep + 1) % 2]

        @pl.loop(2, cx, unroll=2)
        def _(x):
            before, here = pieces(source, x, 0), pieces(source, x, 1)
            for y in range(1, cy - 1):
                after = pieces(source, x, y + 1)
                down, up = pieces(source, x - 1, y), pieces(source, x + 1, y)
                scale = pieces(weight, x - 1, y)
                beside = along_z(here, lane)
                for h in range(parts):
                    total = (down[h] + up[h]) + (before[h] + after[h]) + beside[h]
                    target[x, y, :, h * LANES:(h + 1) * LANES] = (
                        (1.0 - OMEGA) * here[h] + scale[h] * total
                    )
                before, here = here, after

    final = buffers[SWEEPS % 2]
    rows = pl.ds(pl.multiple_of(group * 2 * GROUP, 2 * GROUP), 2 * GROUP)

    @pl.loop(1, cx + 1)
    def _(x):
        before, here = None, pieces(final, x, 0)
        for y in range(cy):
            after = pieces(final, x, y + 1) if y + 1 < cy else None
            down, up = pieces(final, x - 1, y), pieces(final, x + 1, y)
            whole = pieces(centre, x - 1, y)
            beside = along_z(here, lane)
            for h in range(parts):
                total = (down[h] + up[h]) + beside[h]
                if before is not None:
                    total = total + before[h]
                if after is not None:
                    total = total + after[h]
                applied = whole[h] * here[h] - total
                left[x - 1, y * parts + h, rows, :] = halves(here[h])
                right[x - 1, y * parts + h, rows, :] = halves(applied)
            before, here = here, after
        for y in range(0, cy, GROUP):
            extended[:, x - 1, y:y + GROUP, :] = jnp.swapaxes(final[x, y:y + GROUP], 0, 1)

    for x in range(0, cx, GROUP):
        upper[:, x:x + GROUP, :] = jnp.swapaxes(final[x + 1:x + 1 + GROUP, cy - 1], 0, 1)

    @pl.when(group == pl.num_programs(0) - 1)
    def _():
        def add(x, total):
            one = jnp.concatenate([left[x, i] for i in range(cy * parts)], axis=1)
            other = jnp.concatenate([right[x, i] for i in range(cy * parts)], axis=1)
            return total + lax.dot_general(
                one, other, (((1,), (1,)), ((), ())), preferred_element_type=jnp.float32
            )

        size = product.shape[0]
        product[...] = lax.fori_loop(0, cx, add, jnp.zeros((size, size), jnp.float32))


def extend(basis, reaction):
    width, cx, cy, cz = basis.shape
    field = (cx + 2, cy, GROUP, cz)
    factors = pltpu.VMEM((cx, cy * cz // LANES, 2 * width, LANES), jnp.bfloat16)
    block = pl.BlockSpec((GROUP, cx, cy, cz), lambda g: (g, 0, 0, 0))
    return pl.pallas_call(
        extend_kernel,
        grid=(width // GROUP,),
        in_specs=[block, pl.BlockSpec((cx, cy, cz), lambda g: (0, 0, 0))],
        out_specs=[
            block,
            pl.BlockSpec((2 * width, 2 * width), lambda g: (0, 0)),
            pl.BlockSpec((GROUP, cx, cz), lambda g: (g, 0, 0)),
        ],
        out_shape=[
            jax.ShapeDtypeStruct(basis.shape, jnp.float32),
            jax.ShapeDtypeStruct((2 * width, 2 * width), jnp.float32),
            jax.ShapeDtypeStruct((width, cx, cz), jnp.float32),
        ],
        scratch_shapes=[
            pltpu.VMEM(field, jnp.float32),
            pltpu.VMEM(field, jnp.float32),
            pltpu.VMEM((cx, cy, GROUP, cz), jnp.float32),
            pltpu.VMEM((cx, cy, GROUP, cz), jnp.float32),
            factors,
            factors,
        ],
        compiler_params=pltpu.CompilerParams(vmem_limit_bytes=56 * 2**20),
        cost_estimate=pl.CostEstimate(
            flops=60 * basis.size, bytes_accessed=8 * basis.size, transcendentals=0
        ),
    )(basis, reaction)


def face_kernel(basis, face):
    face[...] = basis[:, :, 0, :]


def lower_face(basis):
    width, cx, _, cz = basis.shape
    return pl.pallas_call(
        face_kernel,
        grid=(width // GROUP,),
        in_specs=[pl.BlockSpec((GROUP, cx, GROUP, cz), lambda g: (g, 0, 0, 0))],
        out_specs=pl.BlockSpec((GROUP, cx, cz), lambda g: (g, 0, 0)),
        out_shape=jax.ShapeDtypeStruct((width, cx, cz), jnp.float32),
    )(basis)


def couple(own, other):
    width = own.shape[0]
    return -jnp.dot(
        own.reshape(width, -1),
        other.reshape(width, -1).T,
        precision=lax.Precision.HIGHEST,
        preferred_element_type=jnp.float32,
    )


def packed(block):
    rows = block.shape[0] * block.shape[1] // LANES
    return jnp.concatenate(
        [block[i:i + rows] for i in range(0, block.shape[0], rows)], axis=1
    )


def unpacked(tile, width):
    return jnp.concatenate(
        [tile[:, i:i + width] for i in range(0, LANES, width)], axis=0
    )


def spread_kernel(ngx, ngy, product, plus_x, plus_y, coarse, held, send_y, recv_y, send_x, recv_x):
    gx, gy = lax.axis_index("gx"), lax.axis_index("gy")
    width = plus_x.shape[0]

    barrier = pltpu.get_barrier_semaphore()
    for d in range(1, ngy):
        pl.semaphore_signal(
            barrier, inc=1, device_id=(gx, lax.rem(gy + d, ngy)), device_id_type=pl.DeviceIdType.MESH
        )
    for d in range(1, ngx):
        pl.semaphore_signal(
            barrier, inc=1, device_id=(lax.rem(gx + d, ngx), gy), device_id_type=pl.DeviceIdType.MESH
        )

    span = 2 * GROUP
    rows = jnp.concatenate(
        [product[i:i + GROUP] + product[i + GROUP:i + span] for i in range(0, 2 * width, span)], axis=0
    )
    diag = jnp.concatenate(
        [rows[:, i:i + GROUP] + rows[:, i + GROUP:i + span] for i in range(0, 2 * width, span)], axis=1
    )
    held[gx, gy, 0] = packed(diag)
    held[gx, gy, 1] = packed(plus_x[...])
    held[gx, gy, 2] = packed(plus_y[...])
    for y in range(ngy):
        coarse[y, 1] = jnp.zeros((width, width), jnp.float32)
    coarse[0, 3] = jnp.zeros((width, width), jnp.float32)
    pl.semaphore_wait(barrier, ngx + ngy - 2)

    def over_y(owner, peer):
        piece = held.at[gx, owner]
        return pltpu.make_async_remote_copy(
            src_ref=piece, dst_ref=piece, send_sem=send_y.at[peer], recv_sem=recv_y.at[owner],
            device_id=(gx, peer), device_id_type=pl.DeviceIdType.MESH,
        )

    def over_x(row, peer):
        piece = held.at[row]
        return pltpu.make_async_remote_copy(
            src_ref=piece, dst_ref=piece, send_sem=send_x.at[peer], recv_sem=recv_x.at[row],
            device_id=(peer, gy), device_id_type=pl.DeviceIdType.MESH,
        )

    def unpack(row, owner):
        s = row * ngy + owner
        along_x, along_y = unpacked(held[row, owner, 1], width), unpacked(held[row, owner, 2], width)
        coarse[s, 0] = unpacked(held[row, owner, 0], width)
        coarse[s, 2] = along_x
        coarse[s, 4] = along_y

        @pl.when(row < ngx - 1)
        def _():
            coarse[s + ngy, 1] = along_x.T

        @pl.when(s < ngx * ngy - 1)
        def _():
            coarse[s + 1, 3] = along_y.T

    for d in range(1, ngy):
        over_y(gy, lax.rem(gy + d, ngy)).start()
    for d in range(1, ngy):
        owner = lax.rem(gy + d, ngy)
        over_y(owner, owner).wait_recv()
    for e in range(1, ngx):
        over_x(gx, lax.rem(gx + e, ngx)).start()

    @pl.loop(0, ngy)
    def _(owner):
        unpack(gx, owner)

    @pl.loop(1, ngx)
    def _(e):
        row = lax.rem(gx + e, ngx)
        over_x(row, row).wait_recv()

        @pl.loop(0, ngy)
        def _(owner):
            unpack(row, owner)

    for d in range(1, ngy):
        over_y(gy, lax.rem(gy + d, ngy)).wait_send()
    for e in range(1, ngx):
        over_x(gx, lax.rem(gx + e, ngx)).wait_send()


def spread(product, plus_x, plus_y):
    ngx, ngy = lax.axis_size("gx"), lax.axis_size("gy")
    width = plus_x.shape[0]
    vmem = pl.BlockSpec(memory_space=pltpu.VMEM)
    return pl.pallas_call(
        functools.partial(spread_kernel, ngx, ngy),
        in_specs=[vmem] * 3,
        out_specs=vmem,
        out_shape=jax.ShapeDtypeStruct((ngx * ngy, 5, width, width), jnp.float32),
        scratch_shapes=[
            pltpu.VMEM((ngx, ngy, 3, width * width // LANES, LANES), jnp.float32),
            pltpu.SemaphoreType.DMA((ngy,)),
            pltpu.SemaphoreType.DMA((ngy,)),
            pltpu.SemaphoreType.DMA((ngx,)),
            pltpu.SemaphoreType.DMA((ngx,)),
        ],
        compiler_params=pltpu.CompilerParams(collective_id=0, has_side_effects=True),
    )(product, plus_x, plus_y)


def on_device(basis, reaction):
    right_face = passed_along(basis[:, 0], "gx", -1)
    upper_face = passed_along(lower_face(basis), "gy", -1)
    phi, product, upper = extend(basis, reaction)
    plus_x = couple(basis[:, -1], right_face)
    plus_y = couple(upper, upper_face)
    return (phi, spread(product, plus_x, plus_y))


def solution(mesh):
    placed = (P(None, "gx", "gy", None), P("gx", "gy", None))
    return jax.shard_map(
        on_device,
        mesh=mesh,
        in_specs=placed,
        out_specs=(P(None, "gx", "gy", None), P()),
        check_vma=False,
    )
```

```python
import functools

import jax
import jax.numpy as jnp
from jax import lax
from jax.experimental import pallas as pl
from jax.experimental.pallas import tpu as pltpu
from jax.sharding import PartitionSpec as P

SWEEPS = 4
OMEGA = 0.8
GROUP = 8
LANES = 128


def passed_along(block, axis, distance):
    devices = range(lax.axis_size(axis))
    route = [(i - distance, i) for i in devices if i - distance in devices]
    return lax.ppermute(block, axis, route)


def along_z(field, lane):
    zero = jnp.zeros_like(field[0])
    back = [pltpu.roll(piece, 1, 1) for piece in field]
    ahead = [pltpu.roll(piece, LANES - 1, 1) for piece in field]
    sums = []
    for h in range(len(field)):
        below = jnp.where(lane == 0, back[h - 1] if h else zero, back[h])
        above = jnp.where(lane == LANES - 1, ahead[h + 1] if h + 1 < len(field) else zero, ahead[h])
        sums.append(below + above)
    return sums


def pieces(ref, x, y):
    parts = ref.shape[-1] // LANES
    return [ref[x, y, :, h * LANES:(h + 1) * LANES] for h in range(parts)]


def halves(value):
    high = value.astype(jnp.bfloat16).astype(jnp.float32)
    return jnp.concatenate([value, value - high], axis=0).astype(jnp.bfloat16)


def extend_kernel(basis, reaction, extended, product, upper, first, second, weight, centre, left, right):
    _, cx, cy, cz = basis.shape
    parts = cz // LANES
    group = pl.program_id(0)
    lane = lax.broadcasted_iota(jnp.int32, (GROUP, LANES), 1)

    @pl.when(group == 0)
    def _():
        blank = jnp.zeros((cy, GROUP, cz), jnp.float32)
        for buffer in (first,):
            buffer[0] = blank
            buffer[cx + 1] = blank

        @pl.loop(0, cx)
        def _(x):
            whole = 6.0 + reaction[x]
            scaled = OMEGA / whole
            for y in range(cy):
                centre[x, y] = jnp.broadcast_to(whole[y:y + 1], (GROUP, cz))
                weight[x, y] = jnp.broadcast_to(scaled[y:y + 1], (GROUP, cz))

    @pl.loop(0, cx, unroll=2)
    def _(x):
        for y in range(0, cy, GROUP):
            turned = jnp.swapaxes(basis[:, x, y:y + GROUP, :], 0, 1)
            first[x + 1, y:y + GROUP] = turned
            if y == 0:
                second[x + 1, 0] = turned[0]
            if y == cy - GROUP:
                second[x + 1, cy - 1] = turned[GROUP - 1]

    second[1] = first[1]
    second[cx] = first[cx]

    buffers = (first, second)
    for sweep in range(SWEEPS):
        source, target = buffers[sweep % 2], buffers[(sweep + 1) % 2]

        @pl.loop(2, cx, unroll=7)
        def _(x):
            before, here = pieces(source, x, 0), pieces(source, x, 1)
            for y in range(1, cy - 1):
                after = pieces(source, x, y + 1)
                down, up = pieces(source, x - 1, y), pieces(source, x + 1, y)
                scale = pieces(weight, x - 1, y)
                beside = along_z(here, lane)
                for h in range(parts):
                    total = (down[h] + up[h]) + (before[h] + after[h]) + beside[h]
                    target[x, y, :, h * LANES:(h + 1) * LANES] = (
                        (1.0 - OMEGA) * here[h] + scale[h] * total
                    )
                before, here = here, after

    final = buffers[SWEEPS % 2]
    rows = pl.ds(pl.multiple_of(group * 2 * GROUP, 2 * GROUP), 2 * GROUP)

    @pl.loop(1, cx + 1, unroll=2)
    def _(x):
        before, here = None, pieces(final, x, 0)
        for y in range(cy):
            after = pieces(final, x, y + 1) if y + 1 < cy else None
            down, up = pieces(final, x - 1, y), pieces(final, x + 1, y)
            whole = pieces(centre, x - 1, y)
            beside = along_z(here, lane)
            for h in range(parts):
                total = (down[h] + up[h]) + beside[h]
                if before is not None:
                    total = total + before[h]
                if after is not None:
                    total = total + after[h]
                applied = whole[h] * here[h] - total
                left[x - 1, y * parts + h, rows, :] = halves(here[h])
                right[x - 1, y * parts + h, rows, :] = halves(applied)
            before, here = here, after
        for y in range(0, cy, GROUP):
            extended[:, x - 1, y:y + GROUP, :] = jnp.swapaxes(final[x, y:y + GROUP], 0, 1)

    for x in range(0, cx, GROUP):
        upper[:, x:x + GROUP, :] = jnp.swapaxes(final[x + 1:x + 1 + GROUP, cy - 1], 0, 1)

    @pl.when(group == pl.num_programs(0) - 1)
    def _():
        def add(x, total):
            one = jnp.concatenate([left[x, i] for i in range(cy * parts)], axis=1)
            other = jnp.concatenate([right[x, i] for i in range(cy * parts)], axis=1)
            return total + lax.dot_general(
                one, other, (((1,), (1,)), ((), ())), preferred_element_type=jnp.float32
            )

        size = product.shape[0]
        product[...] = lax.fori_loop(0, cx, add, jnp.zeros((size, size), jnp.float32))


def extend(basis, reaction):
    width, cx, cy, cz = basis.shape
    field = (cx + 2, cy, GROUP, cz)
    factors = pltpu.VMEM((cx, cy * cz // LANES, 2 * width, LANES), jnp.bfloat16)
    block = pl.BlockSpec((GROUP, cx, cy, cz), lambda g: (g, 0, 0, 0))
    return pl.pallas_call(
        extend_kernel,
        grid=(width // GROUP,),
        in_specs=[block, pl.BlockSpec((cx, cy, cz), lambda g: (0, 0, 0))],
        out_specs=[
            block,
            pl.BlockSpec((2 * width, 2 * width), lambda g: (0, 0)),
            pl.BlockSpec((GROUP, cx, cz), lambda g: (g, 0, 0)),
        ],
        out_shape=[
            jax.ShapeDtypeStruct(basis.shape, jnp.float32),
            jax.ShapeDtypeStruct((2 * width, 2 * width), jnp.float32),
            jax.ShapeDtypeStruct((width, cx, cz), jnp.float32),
        ],
        scratch_shapes=[
            pltpu.VMEM(field, jnp.float32),
            pltpu.VMEM(field, jnp.float32),
            pltpu.VMEM((cx, cy, GROUP, cz), jnp.float32),
            pltpu.VMEM((cx, cy, GROUP, cz), jnp.float32),
            factors,
            factors,
        ],
        compiler_params=pltpu.CompilerParams(vmem_limit_bytes=56 * 2**20),
        cost_estimate=pl.CostEstimate(
            flops=60 * basis.size, bytes_accessed=8 * basis.size, transcendentals=0
        ),
    )(basis, reaction)


def face_kernel(basis, face):
    face[...] = basis[:, :, 0, :]


def lower_face(basis):
    width, cx, _, cz = basis.shape
    return pl.pallas_call(
        face_kernel,
        grid=(width // GROUP,),
        in_specs=[pl.BlockSpec((GROUP, cx, GROUP, cz), lambda g: (g, 0, 0, 0))],
        out_specs=pl.BlockSpec((GROUP, cx, cz), lambda g: (g, 0, 0)),
        out_shape=jax.ShapeDtypeStruct((width, cx, cz), jnp.float32),
    )(basis)


def couple(own, other):
    width = own.shape[0]
    return -jnp.dot(
        own.reshape(width, -1),
        other.reshape(width, -1).T,
        precision=lax.Precision.HIGHEST,
        preferred_element_type=jnp.float32,
    )


def packed(block):
    rows = block.shape[0] * block.shape[1] // LANES
    return jnp.concatenate(
        [block[i:i + rows] for i in range(0, block.shape[0], rows)], axis=1
    )


def unpacked(tile, width):
    return jnp.concatenate(
        [tile[:, i:i + width] for i in range(0, LANES, width)], axis=0
    )


def spread_kernel(ngx, ngy, product, plus_x, plus_y, coarse, held, send_y, recv_y, send_x, recv_x):
    gx, gy = lax.axis_index("gx"), lax.axis_index("gy")
    width = plus_x.shape[0]

    barrier = pltpu.get_barrier_semaphore()
    for d in range(1, ngy):
        pl.semaphore_signal(
            barrier, inc=1, device_id=(gx, lax.rem(gy + d, ngy)), device_id_type=pl.DeviceIdType.MESH
        )
    for d in range(1, ngx):
        pl.semaphore_signal(
            barrier, inc=1, device_id=(lax.rem(gx + d, ngx), gy), device_id_type=pl.DeviceIdType.MESH
        )

    span = 2 * GROUP
    rows = jnp.concatenate(
        [product[i:i + GROUP] + product[i + GROUP:i + span] for i in range(0, 2 * width, span)], axis=0
    )
    diag = jnp.concatenate(
        [rows[:, i:i + GROUP] + rows[:, i + GROUP:i + span] for i in range(0, 2 * width, span)], axis=1
    )
    held[gx, gy, 0] = packed(diag)
    held[gx, gy, 1] = packed(plus_x[...])
    held[gx, gy, 2] = packed(plus_y[...])
    for y in range(ngy):
        coarse[y, 1] = jnp.zeros((width, width), jnp.float32)
    coarse[0, 3] = jnp.zeros((width, width), jnp.float32)
    pl.semaphore_wait(barrier, ngx + ngy - 2)

    def over_y(owner, peer):
        piece = held.at[gx, owner]
        return pltpu.make_async_remote_copy(
            src_ref=piece, dst_ref=piece, send_sem=send_y.at[peer], recv_sem=recv_y.at[owner],
            device_id=(gx, peer), device_id_type=pl.DeviceIdType.MESH,
        )

    def over_x(row, owner, peer):
        piece = held.at[row, owner]
        return pltpu.make_async_remote_copy(
            src_ref=piece, dst_ref=piece, send_sem=send_x.at[peer, owner], recv_sem=recv_x.at[row, owner],
            device_id=(peer, gy), device_id_type=pl.DeviceIdType.MESH,
        )

    def unpack(row, owner):
        s = row * ngy + owner
        along_x, along_y = unpacked(held[row, owner, 1], width), unpacked(held[row, owner, 2], width)
        coarse[s, 0] = unpacked(held[row, owner, 0], width)
        coarse[s, 2] = along_x
        coarse[s, 4] = along_y

        @pl.when(row < ngx - 1)
        def _():
            coarse[s + ngy, 1] = along_x.T

        @pl.when(s < ngx * ngy - 1)
        def _():
            coarse[s + 1, 3] = along_y.T

    for d in range(1, ngy):
        over_y(gy, lax.rem(gy + d, ngy)).start()
    for d in range(1, ngx):
        over_x(gx, gy, lax.rem(gx + d, ngx)).start()
    for d in range(1, ngy):
        owner = lax.rem(gy + d, ngy)
        over_y(owner, owner).wait_recv()
        for e in range(1, ngx):
            over_x(gx, owner, lax.rem(gx + e, ngx)).start()

    @pl.loop(0, ngy)
    def _(owner):
        unpack(gx, owner)

    @pl.loop(0, ngy)
    def _(d):
        owner = lax.rem(gy + d, ngy)

        @pl.loop(1, ngx)
        def _(e):
            row = lax.rem(gx + e, ngx)
            over_x(row, owner, row).wait_recv()
            unpack(row, owner)

    for d in range(1, ngy):
        over_y(gy, lax.rem(gy + d, ngy)).wait_send()
    for d in range(ngy):
        owner = lax.rem(gy + d, ngy)
        for e in range(1, ngx):
            over_x(gx, owner, lax.rem(gx + e, ngx)).wait_send()


def spread(product, plus_x, plus_y):
    ngx, ngy = lax.axis_size("gx"), lax.axis_size("gy")
    width = plus_x.shape[0]
    vmem = pl.BlockSpec(memory_space=pltpu.VMEM)
    return pl.pallas_call(
        functools.partial(spread_kernel, ngx, ngy),
        in_specs=[vmem] * 3,
        out_specs=vmem,
        out_shape=jax.ShapeDtypeStruct((ngx * ngy, 5, width, width), jnp.float32),
        scratch_shapes=[
            pltpu.VMEM((ngx, ngy, 3, width * width // LANES, LANES), jnp.float32),
            pltpu.SemaphoreType.DMA((ngy,)),
            pltpu.SemaphoreType.DMA((ngy,)),
            pltpu.SemaphoreType.DMA((ngx, ngy)),
            pltpu.SemaphoreType.DMA((ngx, ngy)),
        ],
        compiler_params=pltpu.CompilerParams(collective_id=0, has_side_effects=True),
    )(product, plus_x, plus_y)


def on_device(basis, reaction):
    right_face = passed_along(basis[:, 0], "gx", -1)
    upper_face = passed_along(lower_face(basis), "gy", -1)
    phi, product, upper = extend(basis, reaction)
    plus_x = couple(basis[:, -1], right_face)
    plus_y = couple(upper, upper_face)
    return (phi, spread(product, plus_x, plus_y))


def solution(mesh):
    placed = (P(None, "gx", "gy", None), P("gx", "gy", None))
    return jax.shard_map(
        on_device,
        mesh=mesh,
        in_specs=placed,
        out_specs=(P(None, "gx", "gy", None), P()),
        check_vma=False,
    )
```
